32 devices in a mesh: aa: 8 (over z, x), ba: 4 (over y, core).
Axes of the slice: x: 2, y: 2, z: 4, core: 2. Of those that a mesh axis runs over, the one named last changes fastest.
Arguments:
- grid_features: bfloat16 [128, 128, 256, 128], P('aa', 'ba'), may hold values from -6 to 6
- weight_real: bfloat16 [32, 32, 16, 128, 128], P('ba', None, 'aa'), may hold values from -6 to 6
- weight_imag: bfloat16 [32, 32, 16, 128, 128], P('ba', None, 'aa'), may hold values from -6 to 6
- mode_keep: int32 [32, 16], P('ba', 'aa'), may hold values from 1 to 16, as said below
- local_weight: bfloat16 [128, 128], replicated, may hold values from -0.5 to 0.5
- local_bias: bfloat16 [128], replicated, may hold values from -3 to 3
Outputs:
- layer_output: bfloat16 [128, 128, 256, 128], P('aa', 'ba')
The draws below stay inside these ranges and needn't reach their ends.
Inputs may be any that keep to these rules, and one draw needn't show every extreme that they name: mode_keep[i, k] counts the retained levels of the second frequency on the line of the i-th retained first frequency and the k-th third frequency.
All inputs are finite; a program needn't handle non-finite values.
Results may differ from the reference program's by a relative error of at most 0.012.
Values may be sent and summed in bfloat16 or wider, within the bound.
A program may use at most 256 MiB of HBM per device.

```python
import math
import jax
import jax.numpy as jnp
from jax import lax

NX = 128
NY = 128
NZ = 256
C = 128
KX = 32
KY = 32
KZ = 16
N_AA = 8


def draw_mode_keep(key, part):
    top_level = KY // 2
    positions = jnp.arange(KX, dtype=jnp.int32)
    level_first = jnp.where(positions < KX // 2, positions, KX - 1 - positions)
    level_third = jnp.arange(KZ, dtype=jnp.int32)
    reach_total = KX // 2 + KZ
    base_level = top_level - (level_first[:, None] + level_third[None, :]) * top_level // reach_total
    jitter = jax.random.randint(key, (KX, KZ), -3, 4, dtype=jnp.int32)
    kept_levels = jnp.clip(base_level + jitter, 1, top_level)
    kept_levels = kept_levels.at[0, 0].set(top_level)
    kept_levels = kept_levels.at[KX // 2 - 1, KZ - 1].set(1)
    return kept_levels.astype(jnp.int32)


def block_levels(own_key, dims, shards, low, top_value):
    def one(dim, shards_of):
        draws = jax.random.uniform(jax.random.fold_in(jax.random.fold_in(own_key, 6), dim), (shards_of,), jnp.float32, low / len(shards), top_value / len(shards))
        return jnp.repeat(jnp.exp(draws), dims[dim] // shards_of).reshape((-1,) + (1,) * (len(dims) - dim - 1))

    gain = one(*shards[0])
    for cut in shards[1:]:
        gain = gain * one(*cut)
    return gain


def centred(rng, extent, spread, limit, pieces=(), kind=jnp.bfloat16):
    drawn = jax.random.normal(rng, extent, jnp.float32) * spread
    if len(pieces) > 0:
        drawn = block_levels(rng, extent, pieces, -0.22, 0.18) * drawn
    return jnp.clip(drawn, min=-limit, max=limit).astype(kind)


def setup_inputs(seed: int = 0) -> dict:
    keys = jax.random.split(jax.random.key(seed), 7)
    grid_features = centred(keys[0], (NX, NY, NZ, C), 1.0, 6.0, ((0, 8), (1, 4)))
    weight_real = centred(keys[1], (KX, KY, KZ, C, C), 1.0, 6.0, ((0, 4), (2, 8)))
    weight_imag = centred(keys[2], (KX, KY, KZ, C, C), 1.0, 6.0, ((0, 4), (2, 8)))
    mode_keep = draw_mode_keep(jax.random.fold_in(keys[6], 71), 0)
    local_weight = centred(keys[4], (C, C), C ** -0.5, 0.5)
    local_bias = centred(keys[5], (C,), 0.5, 3.0)
    return {"grid_features": grid_features, "weight_real": weight_real, "weight_imag": weight_imag, "mode_keep": mode_keep, "local_weight": local_weight, "local_bias": local_bias}


highest = lax.Precision.HIGHEST


def kept_modes(length, number):
    positions = jnp.arange(number, dtype=jnp.int32)
    return jnp.where(positions < number // 2, positions, positions + (length - number)).astype(jnp.int32)


def phase_tables(length, mode_list):
    places = jnp.arange(length, dtype=jnp.int32)
    phase_steps = (places[:, None] * mode_list[None, :]) % length
    angles = phase_steps.astype(jnp.float32) * (2.0 * math.pi / length)
    return jnp.cos(angles), jnp.sin(angles)


def forward_kernel(length, number):
    cosine_table, sine_table = phase_tables(length, kept_modes(length, number))
    upper_rows = jnp.concatenate([cosine_table, -sine_table], axis=1)
    lower_rows = jnp.concatenate([sine_table, cosine_table], axis=1)
    return jnp.concatenate([upper_rows, lower_rows], axis=0)


def inverse_kernel(length, number):
    cosine_table, sine_table = phase_tables(length, kept_modes(length, number))
    upper_rows = jnp.concatenate([cosine_table.T, sine_table.T], axis=1)
    lower_rows = jnp.concatenate([-sine_table.T, cosine_table.T], axis=1)
    return jnp.concatenate([upper_rows, lower_rows], axis=0)


def depth_kernels():
    cosine_table, sine_table = phase_tables(NZ, jnp.arange(KZ, dtype=jnp.int32))
    forward = jnp.concatenate([cosine_table, -sine_table], axis=1).astype(jnp.bfloat16)
    factor = jnp.where(jnp.arange(KZ, dtype=jnp.int32) == 0, 1.0, 2.0).astype(jnp.float32) / (NX * NY * NZ)
    inverse = jnp.concatenate([cosine_table.T * factor[:, None], -sine_table.T * factor[:, None]], axis=0).astype(jnp.bfloat16)
    return forward, inverse


def along_first(operand, kernel):
    return jnp.einsum('pabc,pq->qabc', operand, kernel, precision=highest, preferred_element_type=jnp.float32)


def along_second(operand, kernel):
    return jnp.einsum('apbc,pq->aqbc', operand, kernel, precision=highest, preferred_element_type=jnp.float32)


def mode_mask(kept_counts):
    positions = jnp.arange(KY, dtype=jnp.int32)
    levels = jnp.where(positions < KY // 2, positions, KY - 1 - positions)
    return (levels[None, :, None] < kept_counts[:, None, :]).astype(jnp.float32)


def reference(grid_features, weight_real, weight_imag, mode_keep, local_weight, local_bias):
    forward_depth, inverse_depth = depth_kernels()
    slab_rows = NX // N_AA
    field_slabs = grid_features.reshape(N_AA, slab_rows, NY, NZ, C)

    def depth_forward(slab_cells):
        flat_rows = jnp.transpose(slab_cells, (0, 1, 3, 2)).reshape(slab_rows * NY * C, NZ).astype(jnp.float32)
        coeffs = jnp.dot(flat_rows, forward_depth.astype(jnp.float32), precision=highest, preferred_element_type=jnp.float32)
        coeffs = jnp.transpose(coeffs.reshape(slab_rows, NY, C, 2 * KZ), (0, 1, 3, 2))
        return coeffs.astype(jnp.bfloat16)

    coeffs = lax.map(depth_forward, field_slabs).reshape(NX, NY, 2 * KZ, C)
    stacked = jnp.concatenate([coeffs[:, :, :KZ], coeffs[:, :, KZ:]], axis=0).astype(jnp.float32)
    result = along_first(stacked, forward_kernel(NX, KX))
    result = jnp.concatenate([result[:KX], result[KX:]], axis=1)
    result = along_second(result, forward_kernel(NY, KY)).astype(jnp.bfloat16)
    spec_real = result[:, :KY]
    spec_imag = result[:, KY:]

    def mix_line(operands):
        real_part, imag_part, line_real, line_imag = operands
        real_part = real_part.astype(jnp.float32)
        imag_part = imag_part.astype(jnp.float32)
        line_real = line_real.astype(jnp.float32)
        line_imag = line_imag.astype(jnp.float32)
        pattern = 'bcd,bcde->bce'
        out_real = jnp.einsum(pattern, real_part, line_real, precision=highest) - jnp.einsum(pattern, imag_part, line_imag, precision=highest)
        out_imag = jnp.einsum(pattern, real_part, line_imag, precision=highest) + jnp.einsum(pattern, imag_part, line_real, precision=highest)
        return out_real, out_imag

    mixed_real, mixed_imag = lax.map(mix_line, (spec_real, spec_imag, weight_real, weight_imag))
    keep_mask = mode_mask(mode_keep)[..., None]
    mixed_real = mixed_real * keep_mask
    mixed_imag = mixed_imag * keep_mask
    result = along_second(jnp.concatenate([mixed_real, mixed_imag], axis=1), inverse_kernel(NY, KY))
    result = jnp.concatenate([result[:, :NY], result[:, NY:]], axis=0)
    result = along_first(result, inverse_kernel(NX, KX)).astype(jnp.bfloat16)
    back_field = jnp.concatenate([result[:NX], result[NX:]], axis=2)
    back_slabs = back_field.reshape(N_AA, slab_rows, NY, 2 * KZ, C)

    def finish_slab(operands):
        slab_cells, back_slab = operands
        flat_rows = jnp.transpose(back_slab, (0, 1, 3, 2)).reshape(slab_rows * NY * C, 2 * KZ).astype(jnp.float32)
        spectral = jnp.dot(flat_rows, inverse_depth.astype(jnp.float32), precision=highest, preferred_element_type=jnp.float32)
        spectral = jnp.transpose(spectral.reshape(slab_rows, NY, C, NZ), (0, 1, 3, 2))
        local_term = jnp.dot(slab_cells.reshape(-1, C).astype(jnp.float32), local_weight.astype(jnp.float32), precision=highest, preferred_element_type=jnp.float32)
        local_term = local_term.reshape(slab_rows, NY, NZ, C)
        return jax.nn.gelu(spectral + local_term + local_bias.astype(jnp.float32)).astype(jnp.bfloat16)

    return lax.map(finish_slab, (field_slabs, back_slabs)).reshape(NX, NY, NZ, C)
```

```python
import functools
import math

import jax
import jax.numpy as jnp
from jax import lax
from jax.experimental import pallas as pl
from jax.experimental.pallas import tpu as pltpu
from jax.sharding import PartitionSpec as P

CHUNKS = 2
BF = jnp.bfloat16
F32 = jnp.float32


def kept_modes(length, number, positions):
    return jnp.where(positions < number // 2, positions, positions + (length - number))


def phase_tables(length, places, mode_list):
    phase_steps = places[:, None] * mode_list[None, :] % length
    angles = phase_steps.astype(F32) * (2.0 * math.pi / length)
    return jnp.cos(angles), jnp.sin(angles)


def forward_table(length, places, modes):
    c, s = phase_tables(length, places, modes)
    return jnp.stack([jnp.stack([c, -s], 1), jnp.stack([s, c], 1)], 0).astype(BF)


def inverse_table(length, places, modes):
    c, s = phase_tables(length, places, modes)
    c, s = c.T, s.T
    return jnp.stack([jnp.stack([c, s], 1), jnp.stack([-s, c], 1)], 0).astype(BF)


def depth_body(table_ref, x_ref, out_ref):
    rows = x_ref.shape[1]
    chans = x_ref.shape[3]
    for j in range(rows // 2):
        pair = jnp.concatenate([x_ref[0, 2 * j], x_ref[0, 2 * j + 1]], axis=1)
        res = jnp.dot(table_ref[...], pair, preferred_element_type=F32).astype(BF)
        out_ref[0, 2 * j] = res[:, :chans]
        out_ref[0, 2 * j + 1] = res[:, chans:]


def depth_forward(grid_features, table, first, count):
    _, rows, depth, chans = grid_features.shape
    modes = table.shape[0]
    return pl.pallas_call(
        depth_body,
        grid=(count,),
        in_specs=[
            pl.BlockSpec((modes, depth), lambda i: (0, 0)),
            pl.BlockSpec((1, rows, depth, chans), lambda i: (i + first, 0, 0, 0)),
        ],
        out_specs=pl.BlockSpec((1, rows, modes, chans), lambda i: (i, 0, 0, 0)),
        out_shape=jax.ShapeDtypeStruct((count, rows, modes, chans), BF),
        compiler_params=pltpu.CompilerParams(vmem_limit_bytes=24 << 20),
        cost_estimate=pl.CostEstimate(
            flops=2 * count * rows * depth * chans * modes * 16,
            bytes_accessed=2 * count * rows * depth * chans,
            transcendentals=0,
        ),
    )(table, grid_features)


def final_body(table_ref, w_ref, bias_ref, x_ref, back_ref, *rest):
    out_ref = rest[-1]
    bias = bias_ref[...]
    c1 = math.sqrt(2.0 / math.pi)

    for j in range(x_ref.shape[1]):
        val = jnp.dot(x_ref[0, j], w_ref[...], preferred_element_type=F32)
        val = val + jnp.dot(table_ref[...], back_ref[0, j], preferred_element_type=F32)
        val = val + bias
        inner = val * (c1 + (c1 * 0.044715) * (val * val))
        half = 0.5 * val
        out_ref[0, j] = (half + half * jnp.tanh(inner)).astype(BF)


def finish(grid_features, back, table, weight, bias, first, so_far):
    total, rows, depth, chans = grid_features.shape
    count, _, modes, _ = back.shape
    block = 8
    while rows % block:
        block //= 2
    big = pl.BlockSpec((1, block, depth, chans), lambda i, j: (i + first, j, 0, 0))
    in_specs = [
        pl.BlockSpec((depth, modes), lambda i, j: (0, 0)),
        pl.BlockSpec((chans, chans), lambda i, j: (0, 0)),
        pl.BlockSpec((1, chans), lambda i, j: (0, 0)),
        big,
        pl.BlockSpec((1, block, modes, chans), lambda i, j: (i, j, 0, 0)),
    ]
    operands = [table, weight, bias, grid_features, back]
    aliases = {}
    if so_far is not None:
        in_specs.append(pl.BlockSpec(memory_space=pl.ANY))
        operands.append(so_far)
        aliases = {5: 0}
    return pl.pallas_call(
        final_body,
        grid=(count, rows // block),
        in_specs=in_specs,
        out_specs=big,
        out_shape=jax.ShapeDtypeStruct(grid_features.shape, BF),
        input_output_aliases=aliases,
        compiler_params=pltpu.CompilerParams(vmem_limit_bytes=24 << 20),
        cost_estimate=pl.CostEstimate(
            flops=2 * count * rows * depth * chans * (chans + modes) * 8,
            bytes_accessed=4 * count * rows * depth * chans,
            transcendentals=count * rows * depth * chans,
        ),
    )(*operands)


def per_device(
    n_aa, n_ba, grid_features, weight_real, weight_imag, mode_keep, local_weight, local_bias
):
    n_x, n_y, depth, chans = grid_features.shape
    kx_own, ky, kz_own = weight_real.shape[:3]
    nx, ny = n_x * n_aa, n_y * n_ba
    kx, kz, ky_own = kx_own * n_ba, kz_own * n_aa, ky // n_ba
    bits = n_ba.bit_length() - 1
    me = lax.axis_index("ba")

    c, s = phase_tables(depth, jnp.arange(depth), jnp.arange(kz))
    depth_fwd = jnp.concatenate([c, -s], axis=1).T.astype(BF)
    factor = jnp.where(jnp.arange(kz) == 0, 1.0, 2.0).astype(F32) / (nx * ny * depth)
    depth_inv = jnp.concatenate([c * factor, -s * factor], axis=1).astype(BF)

    order = jnp.arange(n_ba)
    block = jnp.zeros_like(order)
    for bit in range(bits):
        block = block + ((order >> (bits - 1 - bit)) & 1) * (1 << bit)
    block = block ^ me
    ky_pos = (block[:, None] * ky_own + jnp.arange(ky_own)[None, :]).reshape(-1)
    ky_modes = kept_modes(ny, ky, ky_pos)
    own_y = me * n_y + jnp.arange(n_y)
    y_fwd = forward_table(ny, own_y, ky_modes)
    y_inv = inverse_table(ny, own_y, ky_modes)
    x_modes = kept_modes(nx, kx, jnp.arange(kx))
    x_fwd = forward_table(nx, jnp.arange(nx), x_modes)
    x_inv = inverse_table(nx, jnp.arange(nx), x_modes)

    def swap(value, bit):
        return lax.ppermute(value, "ba", [(i, i ^ (1 << bit)) for i in range(n_ba)])

    per = n_x // CHUNKS
    landed = []
    for ch in range(CHUNKS):
        coeffs = depth_forward(grid_features, depth_fwd, ch * per, per)
        coeffs = coeffs.reshape(per, n_y, 2, kz, chans)
        part = jnp.einsum("xypkc,pyrq->qrxkc", coeffs, y_fwd, preferred_element_type=F32)
        for bit in range(bits):
            half = part.shape[0] // 2
            got = swap(part[half:].astype(BF), bit)
            part = part[:half] + got.astype(F32)
        part = part.astype(BF).reshape(ky_own, 2, per, n_aa, kz_own, chans)
        part = jnp.transpose(part, (3, 2, 0, 1, 4, 5))
        landed.append(lax.all_to_all(part, "aa", 0, 0, tiled=True))
    field = jnp.stack(landed, 1).reshape(nx, ky_own, 2, kz_own, chans)
    spec = jnp.einsum("xqpkc,pxrm->mrqkc", field, x_fwd, preferred_element_type=F32).astype(BF)
    spec = spec.reshape(n_ba, kx_own, 2, ky_own, kz_own, chans)
    spec = lax.all_to_all(spec, "ba", 0, 0, tiled=True)
    spec = jnp.transpose(spec, (1, 0, 3, 4, 2, 5)).reshape(kx_own, ky, kz_own, 2, chans)

    pattern = "abcmd,abcde->abcme"
    by_real = jnp.einsum(pattern, spec, weight_real, preferred_element_type=F32)
    by_imag = jnp.einsum(pattern, spec, weight_imag, preferred_element_type=F32)
    out_real = by_real[..., 0, :] - by_imag[..., 1, :]
    out_imag = by_imag[..., 0, :] + by_real[..., 1, :]
    positions = jnp.arange(ky)
    levels = jnp.where(positions < ky // 2, positions, ky - 1 - positions)
    keep = (levels[None, :, None] < mode_keep[:, None, :]).astype(F32)[..., None]
    mixed = jnp.stack([out_real * keep, out_imag * keep], 0).astype(BF)
    mixed = mixed.reshape(2, kx_own, n_ba, ky_own, kz_own, chans)
    mixed = jnp.transpose(mixed, (2, 1, 0, 3, 4, 5))
    mixed = lax.all_to_all(mixed, "ba", 0, 0, tiled=True)
    mixed = mixed.reshape(kx, 2, ky_own, kz_own, chans)
    back = jnp.einsum("mpqkc,pmrx->xqrkc", mixed, x_inv, preferred_element_type=F32).astype(BF)
    back = back.reshape(n_aa, CHUNKS, per, ky_own, 2, kz_own, chans)

    bias = local_bias.astype(F32).reshape(1, chans)
    fields = []
    for ch in range(CHUNKS):
        piece = lax.all_to_all(back[:, ch], "aa", 0, 0, tiled=True)
        piece = jnp.transpose(piece, (2, 3, 1, 0, 4, 5))
        piece = piece.reshape(ky_own, 2, per, kz, chans)
        for bit in reversed(range(bits)):
            piece = jnp.concatenate([piece, swap(piece, bit)], axis=0)
        field = jnp.einsum("qpxkc,pqry->xyrkc", piece, y_inv, preferred_element_type=F32)
        fields.append(field.astype(BF).reshape(per, n_y, 2 * kz, chans))
    result = None
    for ch in range(CHUNKS):
        result = finish(
            grid_features, fields[ch], depth_inv, local_weight, bias, ch * per, result
        )
    return result


def solution(mesh):
    in_specs = (
        P("aa", "ba", None, None),
        P("ba", None, "aa", None, None),
        P("ba", None, "aa", None, None),
        P("ba", "aa"),
        P(),
        P(),
    )
    out_specs = P("aa", "ba", None, None)
    body = functools.partial(per_device, mesh.shape["aa"], mesh.shape["ba"])
    return jax.shard_map(body, mesh=mesh, in_specs=in_specs, out_specs=out_specs, check_vma=False)
```
